32 devices in a mesh: wide: 16 (over z, y, core), narrow: 2 (over x).
Axes of the slice: x: 2, y: 2, z: 4, core: 2. Of those that a mesh axis runs over, the one named last changes fastest.
Arguments:
- query_coords: float32 [3, 32, 16, 32], P(None, ('wide', 'narrow')), may hold values from -1 to 1
- owner_element: int32 [32, 16, 32], P(('wide', 'narrow')), may hold values from 0 to 15
- pair_counts: int32 [32, 32], P(('wide', 'narrow')), may hold values from 0 to 16, as said below
- fields: bfloat16 [512, 8, 1024], P(('wide', 'narrow')), may hold values from -6 to 6
Outputs:
- values: bfloat16 [16, 32, 16, 32], P(None, ('wide', 'narrow'))
The draws below stay inside these ranges and needn't reach their ends.
Inputs may be any that keep to these rules, and one draw needn't show every extreme that they name: `pair_counts`: every count is at most 16, and some pair of devices reaches 16 in every draw.
All inputs are finite; a program needn't handle non-finite values.
Results may differ from the reference program's by a relative error of at most 0.0043.
Values may be sent and summed in bfloat16 or wider, within the bound.
A program may use at most 64 MiB of HBM per device.

```python
import jax
import jax.numpy as jnp
from jax import lax

FIELDS = 16
NODE = 8
E_DEV = 16
CAP = 16
ELEMS = 512
DEVICES = 32


def draw_pair_counts(key, part):
    key_shift, key_hot, key_count, key_sender = jax.random.split(key, 4)
    shifts = jax.random.randint(key_shift, (DEVICES,), 0, 2)
    hottest = jax.random.randint(key_hot, (), 0, DEVICES)
    owners = jnp.arange(DEVICES)
    shifts = jnp.where(owners == hottest, 0, shifts)
    limits = jnp.maximum(jnp.right_shift(jnp.full((DEVICES,), CAP, jnp.int32), shifts.astype(jnp.int32)), 1)
    lowest = limits // 2
    raw_bits = jax.random.randint(key_count, (DEVICES, DEVICES), 0, 1 << 20)
    counts = lowest[None, :] + raw_bits % (limits[None, :] - lowest[None, :] + 1)
    sender = jax.random.randint(key_sender, (), 0, DEVICES)
    senders = jnp.arange(DEVICES)
    counts = jnp.where((senders[:, None] == sender) & (owners[None, :] == hottest), CAP, counts)
    return counts.astype(jnp.int32)


def with_ends(array, stream_key, low, high):
    spot = [jax.random.randint(jax.random.fold_in(stream_key, axis), (), 0, length) for axis, length in enumerate(array.shape)]
    longest = array.shape.index(max(array.shape))
    beside = spot[:longest] + [(spot[longest] + 1) % array.shape[longest]] + spot[longest + 1:]
    return array.at[tuple(spot)].set(low).at[tuple(beside)].set(high)


def shard_levels(own_key, extent, pieces, smallest, top_value):
    def one(axis_at, blocks):
        steps = jax.random.uniform(jax.random.fold_in(jax.random.fold_in(own_key, 6), axis_at), (blocks,), jnp.float32, smallest / len(pieces), top_value / len(pieces))
        return jnp.repeat(jnp.exp(steps), extent[axis_at] // blocks).reshape((-1,) + (1,) * (len(extent) - axis_at - 1))

    level = one(*pieces[0])
    for cut in pieces[1:]:
        level = level * one(*cut)
    return level


def centred(own_key, shape, spread, reach, cuts=(), kind=jnp.bfloat16):
    array = spread * jax.random.normal(own_key, shape, jnp.float32)
    if cuts:
        array = array * shard_levels(own_key, shape, cuts, -0.22, 0.18)
    return jnp.clip(array, -reach, reach).astype(kind)


def setup_inputs(seed: int = 0) -> dict:
    seeds = jax.random.split(jax.random.key(seed), 5)
    return {
        "query_coords": jnp.clip(jax.random.uniform(seeds[0], (3, DEVICES, CAP, DEVICES), jnp.float32, -1.0, 1.0) * shard_levels(seeds[0], (3, DEVICES, CAP, DEVICES), ((1, 32),), -0.4, 0.0), -1.0, 1.0),
        "owner_element": with_ends(jax.random.randint(seeds[1], (DEVICES, CAP, DEVICES), 0, E_DEV), jax.random.fold_in(seeds[1], 1), 0, E_DEV - 1).astype(jnp.int32),
        "pair_counts": draw_pair_counts(jax.random.fold_in(seeds[4], 71), 0),
        "fields": centred(seeds[3], (ELEMS, NODE, FIELDS * NODE * NODE), 1.0, 6.0, ((0, 32),)),
    }


GLL_NODES = (-1.0, -0.8717401485096066, -0.5917001814331423, -0.2092992179024789, 0.2092992179024789, 0.5917001814331423, 0.8717401485096066, 1.0)


def lagrange(position):
    result = []
    for i in range(8):
        factor = jnp.ones_like(position)
        for m in range(8):
            if m != i:
                factor = factor * ((position - GLL_NODES[m]) / (GLL_NODES[i] - GLL_NODES[m]))
        result.append(factor)
    return jnp.stack(result)


def reference(query_coords, owner_element, pair_counts, fields):
    field_table = fields.reshape(DEVICES, E_DEV, NODE, FIELDS * NODE * NODE)

    def one_owner(owner_index):
        coords_here = lax.dynamic_index_in_dim(query_coords, owner_index, 3, keepdims=False)
        element_here = lax.dynamic_index_in_dim(owner_element, owner_index, 2, keepdims=False)
        counts_here = lax.dynamic_index_in_dim(pair_counts, owner_index, 1, keepdims=False)
        owned = lax.dynamic_index_in_dim(field_table, owner_index, 0, keepdims=False)

        def one_slot(slot_index):
            picked_coords = lax.dynamic_index_in_dim(coords_here, slot_index, 2, keepdims=False)
            element_ids = lax.dynamic_index_in_dim(element_here, slot_index, 1, keepdims=False)
            live = slot_index < counts_here
            basis_r = lagrange(picked_coords[0]).astype(jnp.bfloat16).astype(jnp.float32)
            tensor_st = (lagrange(picked_coords[1])[:, None, :] * lagrange(picked_coords[2])[None, :, :]).reshape(NODE * NODE, -1)
            gathered = owned[element_ids].astype(jnp.float32)
            partial_value = jnp.einsum('sin,is->sn', gathered, basis_r)
            summed = jnp.sum(partial_value.reshape(-1, FIELDS, NODE * NODE) * tensor_st.T[:, None, :], axis=-1)
            return jnp.where(live[:, None], summed, jnp.float32(0.0)).astype(jnp.bfloat16).T

        return lax.map(one_slot, jnp.arange(CAP, dtype=jnp.int32))

    stacked = lax.map(one_owner, jnp.arange(DEVICES, dtype=jnp.int32))
    return jnp.transpose(stacked, (2, 3, 1, 0))
```

```python
import functools
import math

import jax
import jax.numpy as jnp
from jax import lax
from jax.experimental import pallas as pl
from jax.experimental.pallas import tpu as pltpu
from jax.sharding import PartitionSpec as P

GLL_NODES = (
    -1.0,
    -0.8717401485096066,
    -0.5917001814331423,
    -0.2092992179024789,
    0.2092992179024789,
    0.5917001814331423,
    0.8717401485096066,
    1.0,
)
NODE = len(GLL_NODES)
SCALES = tuple(
    1.0 / math.prod(GLL_NODES[i] - GLL_NODES[m] for m in range(NODE) if m != i)
    for i in range(NODE)
)
LANES = 128
MESH = pl.DeviceIdType.MESH


def lagrange_rows(row, node_index, scale):
    position = jnp.broadcast_to(row, (NODE, row.shape[1]))
    factors = [
        jnp.where(node_index == m, 1.0, position - GLL_NODES[m]) for m in range(NODE)
    ]
    while len(factors) > 1:
        factors = [a * b for a, b in zip(factors[::2], factors[1::2])]
    return factors[0] * scale


def kernel(
    sizes,
    coords_hbm,
    element_hbm,
    counts_hbm,
    fields_hbm,
    out_ref,
    coords,
    element,
    counts,
    fields,
    fields_t,
    send_query,
    recv_query,
    send_value,
    recv_value,
    local_sems,
    sems,
):
    wide_size, narrow_size, slots, elements, field_count = sizes
    n = wide_size * narrow_size
    width = min(n, LANES)
    packed = LANES // width
    groups = slots // packed
    me = lax.axis_index("wide") * narrow_size + lax.axis_index("narrow")

    def partner(step):
        offset = n // 2 + (1 - 2 * (step % 2)) * ((step + 1) // 2)
        index = lax.rem(me + offset, n)
        return index, (index // narrow_size, lax.rem(index, narrow_size))

    def for_partners(body):
        if n <= 64:
            for step in range(n - 1):
                body(step)
        else:
            lax.fori_loop(0, n - 1, lambda step, c: (body(step), c)[1], 0)

    loads = [
        pltpu.make_async_copy(src, dst, local_sems.at[i])
        for i, (src, dst) in enumerate(
            (
                (coords_hbm, coords),
                (element_hbm, element),
                (counts_hbm, counts),
                (fields_hbm, fields),
            )
        )
    ]
    for load in loads:
        load.start()
    barrier = pltpu.get_barrier_semaphore()

    def greet(step):
        pl.semaphore_signal(
            barrier, inc=1, device_id=partner(step)[1], device_id_type=MESH
        )

    for_partners(greet)

    for load in loads[:3]:
        load.wait()
    slot_index = lax.broadcasted_iota(jnp.int32, (slots, n), 0)
    picked = jnp.where(slot_index < counts[...], element[...], elements).astype(
        jnp.float32
    )
    pieces = []
    for k in range(packed):
        rows = slice(k * groups, (k + 1) * groups)
        pieces += [coords[0, rows], coords[1, rows], coords[2, rows], picked[rows]]
    payload = jnp.concatenate(pieces, axis=0)
    payload = jnp.concatenate(
        [payload, jnp.zeros((LANES - payload.shape[0], n), jnp.float32)], axis=0
    )
    if n < LANES:
        payload = jnp.concatenate(
            [payload, jnp.zeros((LANES, LANES - n), jnp.float32)], axis=1
        )
    send_query[0] = jnp.transpose(payload)[:n]

    pl.semaphore_wait(barrier, n - 1)

    def exchange(source, target, send_sem, recv_sem, own_sem):
        def send(step):
            index, device = partner(step)
            pltpu.make_async_remote_copy(
                src_ref=source.at[:, pl.ds(index, 1)],
                dst_ref=target.at[:, pl.ds(me, 1)],
                send_sem=send_sem,
                recv_sem=recv_sem,
                device_id=device,
                device_id_type=MESH,
            ).start()

        for_partners(send)
        pltpu.make_async_copy(
            source.at[:, pl.ds(me, 1)], target.at[:, pl.ds(me, 1)], own_sem
        ).start()

    def finish(source, target, recv_sem, own_sem):
        rest = pl.ds(0, n - 1)
        pltpu.make_async_copy(
            source.at[:, rest], target.at[:, rest], recv_sem
        ).wait()
        pltpu.make_async_copy(
            source.at[:, pl.ds(me, 1)], target.at[:, pl.ds(me, 1)], own_sem
        ).wait()

    exchange(send_query, recv_query, sems.at[0], sems.at[1], sems.at[2])

    loads[3].wait()
    fields_t[...] = jnp.transpose(
        fields[...].reshape(elements * NODE, fields.shape[2])
    )
    node_index = lax.broadcasted_iota(jnp.int32, (NODE, LANES), 0)
    scale = jnp.zeros((NODE, LANES), jnp.float32)
    for i in range(NODE):
        scale = jnp.where(node_index == i, jnp.float32(SCALES[i]), scale)

    finish(send_query, recv_query, sems.at[1], sems.at[2])

    def evaluate(block):
        rows = pl.ds(block * width, width)
        arrived = recv_query[0, rows]
        if width < LANES:
            arrived = jnp.concatenate(
                [arrived, jnp.zeros((LANES - width, LANES), jnp.float32)], axis=0
            )
        turned = jnp.transpose(arrived)[:, :width]
        span = 4 * groups
        queries = jnp.concatenate(
            [turned[k * span : (k + 1) * span] for k in range(packed)], axis=1
        )
        results = []
        for g in range(groups):
            r, s, t, e = (queries[c * groups + g :][:1] for c in range(4))
            basis_r = lagrange_rows(r, node_index, scale)
            basis_s = lagrange_rows(s, node_index, scale)
            basis_t = lagrange_rows(t, node_index, scale)
            owner = jnp.broadcast_to(e, (NODE, LANES))
            weights = jnp.concatenate(
                [jnp.where(owner == float(a), basis_r, 0.0) for a in range(elements)],
                axis=0,
            ).astype(jnp.bfloat16)
            tensor = [basis_s[j : j + 1] * basis_t for j in range(NODE)]
            partial = jnp.dot(
                fields_t[...], weights, preferred_element_type=jnp.float32
            )
            for c in range(field_count):
                base = c * NODE * NODE
                total = partial[base : base + NODE] * tensor[0]
                for j in range(1, NODE):
                    at = base + j * NODE
                    total += partial[at : at + NODE] * tensor[j]
                results.append(jnp.sum(total, axis=0, keepdims=True))
        result = jnp.concatenate(results, axis=0)
        back = jnp.transpose(result)
        back = jnp.concatenate(
            [back[k * width : (k + 1) * width] for k in range(packed)], axis=1
        )
        for h in range(back.shape[1] // LANES):
            send_value[h, rows] = back[:, h * LANES : (h + 1) * LANES]

    if n <= LANES:
        evaluate(0)
    else:
        lax.fori_loop(0, n // width, lambda b, c: (evaluate(b), c)[1], 0)

    exchange(send_value, recv_value, sems.at[3], sems.at[4], sems.at[5])

    cells = field_count * slots
    row = lax.broadcasted_iota(jnp.int32, (cells, cells), 0)
    lane = lax.broadcasted_iota(jnp.int32, (cells, cells), 1)
    source = (row % slots) * field_count + row // slots
    order = (lane == source).astype(jnp.float32).astype(jnp.bfloat16)

    finish(send_value, recv_value, sems.at[4], sems.at[5])

    gathered = jnp.concatenate(
        [recv_value[h] for h in range(cells // LANES)], axis=1
    ).astype(jnp.bfloat16)
    values = lax.dot_general(
        order, gathered, (((1,), (1,)), ((), ())), preferred_element_type=jnp.float32
    )
    out_ref[...] = values.astype(jnp.bfloat16).reshape(field_count, slots, n)
    rest = pl.ds(0, n - 1)
    for buffer, other, sem in (
        (send_query, recv_query, sems.at[0]),
        (send_value, recv_value, sems.at[3]),
    ):
        pltpu.make_async_copy(buffer.at[:, rest], other.at[:, rest], sem).wait()


def solution(mesh):
    def on_device(query_coords, owner_element, pair_counts, fields):
        wide_size, narrow_size = mesh.shape["wide"], mesh.shape["narrow"]
        n = wide_size * narrow_size
        slots = owner_element.shape[1]
        elements, node, columns = fields.shape
        field_count = columns // (node * node)
        cells = field_count * slots
        sizes = (wide_size, narrow_size, slots, elements, field_count)
        values = pl.pallas_call(
            functools.partial(kernel, sizes),
            out_shape=jax.ShapeDtypeStruct((field_count, slots, n), jnp.bfloat16),
            in_specs=[pl.BlockSpec(memory_space=pl.ANY)] * 4,
            out_specs=pl.BlockSpec(memory_space=pltpu.VMEM),
            scratch_shapes=[
                pltpu.VMEM((3, slots, n), jnp.float32),
                pltpu.VMEM((slots, n), jnp.int32),
                pltpu.VMEM((1, n), jnp.int32),
                pltpu.VMEM(fields.shape, jnp.bfloat16),
                pltpu.VMEM((columns, elements * node), jnp.bfloat16),
                pltpu.VMEM((1, n, LANES), jnp.float32),
                pltpu.VMEM((1, n, LANES), jnp.float32),
                pltpu.VMEM((cells // LANES, n, LANES), jnp.float32),
                pltpu.VMEM((cells // LANES, n, LANES), jnp.float32),
                pltpu.SemaphoreType.DMA((4,)),
                pltpu.SemaphoreType.DMA((6,)),
            ],
            compiler_params=pltpu.CompilerParams(
                collective_id=0, has_side_effects=True
            ),
            name="exchange_and_evaluate",
        )(query_coords[:, 0], owner_element[0], pair_counts, fields)
        return values[:, None]

    placed = (
        P(None, ("wide", "narrow"), None, None),
        P(("wide", "narrow"), None, None),
        P(("wide", "narrow"), None),
        P(("wide", "narrow"), None, None),
    )
    return jax.shard_map(
        on_device,
        mesh=mesh,
        in_specs=placed,
        out_specs=P(None, ("wide", "narrow"), None, None),
        check_vma=False,
    )
```

```python
import functools
import math

import jax
import jax.numpy as jnp
from jax import lax
from jax.experimental import pallas as pl
from jax.experimental.pallas import tpu as pltpu
from jax.sharding import PartitionSpec as P

GLL_NODES = (
    -1.0,
    -0.8717401485096066,
    -0.5917001814331423,
    -0.2092992179024789,
    0.2092992179024789,
    0.5917001814331423,
    0.8717401485096066,
    1.0,
)
NODE = len(GLL_NODES)
SCALES = tuple(
    1.0 / math.prod(GLL_NODES[i] - GLL_NODES[m] for m in range(NODE) if m != i)
    for i in range(NODE)
)
LANES = 128
MESH = pl.DeviceIdType.MESH


def lagrange_rows(row, node_index, scale):
    position = jnp.broadcast_to(row, (NODE, row.shape[1]))
    factors = [
        jnp.where(node_index == m, 1.0, position - GLL_NODES[m]) for m in range(NODE)
    ]
    while len(factors) > 1:
        factors = [a * b for a, b in zip(factors[::2], factors[1::2])]
    return factors[0] * scale


def kernel(
    sizes,
    coords_hbm,
    element_hbm,
    counts_hbm,
    fields_hbm,
    recv_value,
    coords,
    element,
    counts,
    fields,
    fields_t,
    send_query,
    recv_query,
    send_value,
    local_sems,
    sems,
):
    wide_size, narrow_size, slots, elements, field_count = sizes
    n = wide_size * narrow_size
    width = min(n, LANES)
    packed = LANES // width
    groups = slots // packed
    me = lax.axis_index("wide") * narrow_size + lax.axis_index("narrow")

    def flipped(value, size):
        options = [value]
        bit = 1
        while bit < size:
            turn = bit * (1 - 2 * (value // bit % 2))
            options += [option + turn for option in options]
            bit *= 2
        return options

    mirrored = n <= 64 and n & (n - 1) == 0
    if mirrored:
        wide_options = flipped(lax.axis_index("wide"), wide_size)
        narrow_options = flipped(lax.axis_index("narrow"), narrow_size)

    def partner(step):
        if mirrored:
            mask = n - 1 - step
            wide = wide_options[mask // narrow_size]
            narrow = narrow_options[mask % narrow_size]
            return wide * narrow_size + narrow, (wide, narrow)
        offset = n // 2 + (1 - 2 * (step % 2)) * ((step + 1) // 2)
        index = lax.rem(me + offset, n)
        return index, (index // narrow_size, lax.rem(index, narrow_size))

    def for_partners(body):
        if n <= 64:
            for step in range(n - 1):
                body(step)
        else:
            lax.fori_loop(0, n - 1, lambda step, c: (body(step), c)[1], 0)

    loads = [
        pltpu.make_async_copy(src, dst, local_sems.at[i])
        for i, (src, dst) in enumerate(
            (
                (coords_hbm, coords),
                (element_hbm, element),
                (counts_hbm, counts),
                (fields_hbm, fields),
            )
        )
    ]
    for load in loads:
        load.start()
    barrier = pltpu.get_barrier_semaphore()

    def greet(step):
        pl.semaphore_signal(
            barrier, inc=1, device_id=partner(step)[1], device_id_type=MESH
        )

    for_partners(greet)

    for load in loads[:3]:
        load.wait()
    slot_index = lax.broadcasted_iota(jnp.int32, (slots, n), 0)
    picked = jnp.where(slot_index < counts[...], element[...], elements).astype(
        jnp.float32
    )
    pieces = []
    for k in range(packed):
        rows = slice(k * groups, (k + 1) * groups)
        pieces += [coords[0, rows], coords[1, rows], coords[2, rows], picked[rows]]
    payload = jnp.concatenate(pieces, axis=0)
    payload = jnp.concatenate(
        [payload, jnp.zeros((LANES - payload.shape[0], n), jnp.float32)], axis=0
    )
    if n < LANES:
        payload = jnp.concatenate(
            [payload, jnp.zeros((LANES, LANES - n), jnp.float32)], axis=1
        )
    send_query[0] = jnp.transpose(payload)[:n]

    pl.semaphore_wait(barrier, n - 1)

    def exchange(source, target, send_sem, recv_sem, own_sem):
        def send(step):
            index, device = partner(step)
            pltpu.make_async_remote_copy(
                src_ref=source.at[:, pl.ds(index, 1)],
                dst_ref=target.at[:, pl.ds(me, 1)],
                send_sem=send_sem,
                recv_sem=recv_sem,
                device_id=device,
                device_id_type=MESH,
            ).start()

        for_partners(send)
        pltpu.make_async_copy(
            source.at[:, pl.ds(me, 1)], target.at[:, pl.ds(me, 1)], own_sem
        ).start()

    def finish(source, target, recv_sem, own_sem):
        rest = pl.ds(0, n - 1)
        pltpu.make_async_copy(
            source.at[:, rest], target.at[:, rest], recv_sem
        ).wait()
        pltpu.make_async_copy(
            source.at[:, pl.ds(me, 1)], target.at[:, pl.ds(me, 1)], own_sem
        ).wait()

    exchange(send_query, recv_query, sems.at[0], sems.at[1], sems.at[2])

    loads[3].wait()
    fields_t[...] = jnp.transpose(
        fields[...].reshape(elements * NODE, fields.shape[2])
    )
    node_index = lax.broadcasted_iota(jnp.int32, (NODE, LANES), 0)
    scale = jnp.zeros((NODE, LANES), jnp.float32)
    for i in range(NODE):
        scale = jnp.where(node_index == i, jnp.float32(SCALES[i]), scale)

    finish(send_query, recv_query, sems.at[1], sems.at[2])

    def evaluate(block):
        rows = pl.ds(block * width, width)
        arrived = recv_query[0, rows]
        if width < LANES:
            arrived = jnp.concatenate(
                [arrived, jnp.zeros((LANES - width, LANES), jnp.float32)], axis=0
            )
        turned = jnp.transpose(arrived)[:, :width]
        span = 4 * groups
        queries = jnp.concatenate(
            [turned[k * span : (k + 1) * span] for k in range(packed)], axis=1
        )
        results = []
        for g in range(groups):
            r, s, t, e = (queries[c * groups + g :][:1] for c in range(4))
            basis_r = lagrange_rows(r, node_index, scale)
            basis_s = lagrange_rows(s, node_index, scale)
            basis_t = lagrange_rows(t, node_index, scale)
            owner = jnp.broadcast_to(e, (NODE, LANES))
            weights = jnp.concatenate(
                [jnp.where(owner == float(a), basis_r, 0.0) for a in range(elements)],
                axis=0,
            ).astype(jnp.bfloat16)
            tensor = [basis_s[j : j + 1] * basis_t for j in range(NODE)]
            partial = jnp.dot(
                fields_t[...], weights, preferred_element_type=jnp.float32
            )
            for c in range(field_count):
                base = c * NODE * NODE
                total = partial[base : base + NODE] * tensor[0]
                for j in range(1, NODE):
                    at = base + j * NODE
                    total += partial[at : at + NODE] * tensor[j]
                results.append(jnp.sum(total, axis=0, keepdims=True))
        result = jnp.concatenate(results, axis=0)
        back = jnp.transpose(result)
        back = jnp.concatenate(
            [back[k * width : (k + 1) * width] for k in range(packed)], axis=1
        )
        for h in range(back.shape[1] // LANES):
            send_value[h, rows] = back[:, h * LANES : (h + 1) * LANES]

    if n <= LANES:
        evaluate(0)
    else:
        lax.fori_loop(0, n // width, lambda b, c: (evaluate(b), c)[1], 0)

    exchange(send_value, recv_value, sems.at[3], sems.at[4], sems.at[5])

    finish(send_value, recv_value, sems.at[4], sems.at[5])

    rest = pl.ds(0, n - 1)
    for buffer, other, sem in (
        (send_query, recv_query, sems.at[0]),
        (send_value, recv_value, sems.at[3]),
    ):
        pltpu.make_async_copy(buffer.at[:, rest], other.at[:, rest], sem).wait()


def unpack(sizes, received, out_ref, recv_value, sem):
    field_count, slots, n = sizes
    load = pltpu.make_async_copy(received, recv_value, sem)
    load.start()
    cells = field_count * slots
    row = lax.broadcasted_iota(jnp.int32, (cells, cells), 0)
    lane = lax.broadcasted_iota(jnp.int32, (cells, cells), 1)
    source = (row % slots) * field_count + row // slots
    order = (lane == source).astype(jnp.float32).astype(jnp.bfloat16)

    load.wait()
    gathered = jnp.concatenate(
        [recv_value[h] for h in range(cells // LANES)], axis=1
    ).astype(jnp.bfloat16)
    values = lax.dot_general(
        order, gathered, (((1,), (1,)), ((), ())), preferred_element_type=jnp.float32
    )
    out_ref[...] = values.astype(jnp.bfloat16).reshape(field_count, slots, n)


def solution(mesh):
    def on_device(query_coords, owner_element, pair_counts, fields):
        wide_size, narrow_size = mesh.shape["wide"], mesh.shape["narrow"]
        n = wide_size * narrow_size
        slots = owner_element.shape[1]
        elements, node, columns = fields.shape
        field_count = columns // (node * node)
        cells = field_count * slots
        sizes = (wide_size, narrow_size, slots, elements, field_count)
        received = pl.pallas_call(
            functools.partial(kernel, sizes),
            out_shape=jax.ShapeDtypeStruct((cells // LANES, n, LANES), jnp.float32),
            in_specs=[pl.BlockSpec(memory_space=pl.ANY)] * 4,
            out_specs=pl.BlockSpec(memory_space=pl.ANY),
            scratch_shapes=[
                pltpu.VMEM((3, slots, n), jnp.float32),
                pltpu.VMEM((slots, n), jnp.int32),
                pltpu.VMEM((1, n), jnp.int32),
                pltpu.VMEM(fields.shape, jnp.bfloat16),
                pltpu.VMEM((columns, elements * node), jnp.bfloat16),
                pltpu.VMEM((1, n, LANES), jnp.float32),
                pltpu.VMEM((1, n, LANES), jnp.float32),
                pltpu.VMEM((cells // LANES, n, LANES), jnp.float32),
                pltpu.SemaphoreType.DMA((4,)),
                pltpu.SemaphoreType.DMA((6,)),
            ],
            compiler_params=pltpu.CompilerParams(
                collective_id=0, has_side_effects=True
            ),
            name="exchange_and_evaluate",
        )(query_coords[:, 0], owner_element[0], pair_counts, fields)
        values = pl.pallas_call(
            functools.partial(unpack, (field_count, slots, n)),
            out_shape=jax.ShapeDtypeStruct((field_count, slots, n), jnp.bfloat16),
            in_specs=[pl.BlockSpec(memory_space=pl.ANY)],
            out_specs=pl.BlockSpec(memory_space=pltpu.VMEM),
            scratch_shapes=[
                pltpu.VMEM(received.shape, received.dtype),
                pltpu.SemaphoreType.DMA,
            ],
            name="unpack",
        )(received)
        return values[:, None]

    placed = (
        P(None, ("wide", "narrow"), None, None),
        P(("wide", "narrow"), None, None),
        P(("wide", "narrow"), None),
        P(("wide", "narrow"), None, None),
    )
    return jax.shard_map(
        on_device,
        mesh=mesh,
        in_specs=placed,
        out_specs=P(None, ("wide", "narrow"), None, None),
        check_vma=False,
    )
```
